32 devices in a mesh: ctx: 2 (over x), tp: 4 (over y, core), dp: 4 (over z).
Axes of the slice: x: 2, y: 2, z: 4, core: 2. Of those that a mesh axis runs over, the one named last changes fastest.
Arguments:
- hidden: bfloat16 [4, 1024, 4096], P('dp', 'ctx', 'tp'), may hold values from -6 to 6
- target: bfloat16 [4, 1024, 4096], P('dp', 'ctx', 'tp'), may hold values from -24 to 24
- gain: float32 [4096], replicated, may hold values from 0.5 to 1.5
- w_query: bfloat16 [4096, 2048], P(('ctx', 'dp'), 'tp'), may hold values from -2.15625 to 2.15625
- w_key: bfloat16 [4096, 512], P(('ctx', 'dp'), 'tp'), may hold values from -0.09375 to 0.09375
- value_matrix: bfloat16 [4096, 512], P(('ctx', 'dp'), 'tp'), may hold values from -0.09375 to 0.09375
- w_out: bfloat16 [2048, 4096], P('tp', ('ctx', 'dp')), may hold values from -0.125 to 0.125
- block_order: int32 [4], replicated, may hold values from 0 to 3, each once
Outputs:
- branch: bfloat16 [4, 1024, 4096], P('dp', 'ctx', 'tp')
- loss: float32 [], replicated
The draws below stay inside these ranges and needn't reach their ends.
Inputs may be any that keep to these rules, and one draw needn't show every extreme that they name: block_order is a permutation of 0 to 3.
All inputs are finite; a program needn't handle non-finite values.
Results may differ from the reference program's by a relative error of at most 0.013.
The reference program's roundings to bfloat16 on the way (of `normed` and `attn`) count: a program that leaves them out, or rounds other values in their place, can miss the bound.
Values may be sent and summed in bfloat16 or wider, within the bound.
A program may use at most 128 MiB of HBM per device.

```python
import math
import jax
import jax.numpy as jnp
from jax import lax

MODEL_WIDTH = 4096
QUERY_HEADS = 16
KEY_VALUE_HEADS = 4
HEAD_SIZE = 128
CH = 256
SEQUENCE_LENGTH = 1024
SEQS = 4
N_CTX = 2
N_TP = 4


def key_weights(key):
    random_jitter = jax.random.normal(jax.random.fold_in(key, 11), (MODEL_WIDTH, KEY_VALUE_HEADS * HEAD_SIZE), jnp.float32)
    return jnp.clip(random_jitter, -6.0, 6.0) / MODEL_WIDTH ** 0.5


def draw_w_key(key, part):
    return key_weights(key).astype(jnp.bfloat16)


def draw_w_query(key, part):
    random_jitter = jax.random.normal(jax.random.fold_in(key, 23), (MODEL_WIDTH, QUERY_HEADS * HEAD_SIZE), jnp.float32)
    base = jnp.clip(random_jitter, -6.0, 6.0) * (3.0 / MODEL_WIDTH ** 0.5)
    return base.astype(jnp.bfloat16)


def draw_hidden(key, part):
    base = jnp.clip(jax.random.normal(jax.random.fold_in(key, 41), (SEQS, SEQUENCE_LENGTH, MODEL_WIDTH), jnp.float32), -6.0, 6.0)
    return base.astype(jnp.bfloat16)


def draw_target(key, part):
    fraction = jnp.arange(SEQUENCE_LENGTH, dtype=jnp.float32) / (SEQUENCE_LENGTH - 1)
    scale = jnp.exp(fraction * jnp.log(6.0))
    noise = jnp.clip(jax.random.normal(jax.random.fold_in(key, 67), (SEQS, SEQUENCE_LENGTH, MODEL_WIDTH), jnp.float32), -4.0, 4.0)
    return jnp.clip(noise * scale[None, :, None], -24.0, 24.0).astype(jnp.bfloat16)


def shard_levels(rng, extent, cuts, least, largest):
    def one(dim, shards_of):
        steps = jax.random.uniform(jax.random.fold_in(jax.random.fold_in(rng, 6), dim), (shards_of,), jnp.float32, least / len(cuts), largest / len(cuts))
        return jnp.repeat(jnp.exp(steps), extent[dim] // shards_of).reshape((-1,) + (1,) * (len(extent) - dim - 1))

    factor_of = one(*cuts[0])
    for cut in cuts[1:]:
        factor_of = factor_of * one(*cut)
    return factor_of


def normal_values(own_key, extent, scale, bound, shards=(), kind=jnp.bfloat16):
    values = scale * jax.random.normal(own_key, extent, jnp.float32)
    if shards:
        values = values * shard_levels(own_key, extent, shards, -0.22, 0.18)
    return jnp.clip(values, -bound, bound).astype(kind)


def setup_inputs(seed: int = 0) -> dict:
    seeds = jax.random.split(jax.random.key(seed), 9)
    hidden = draw_hidden(jax.random.fold_in(seeds[8], 71), 0)
    target = draw_target(jax.random.fold_in(seeds[8], 71), 0)
    gain = jnp.clip(1.0 + 0.1 * jax.random.normal(seeds[2], (MODEL_WIDTH,), jnp.float32), 0.5, 1.5)
    w_query = draw_w_query(jax.random.fold_in(seeds[8], 71), 0)
    w_key = draw_w_key(jax.random.fold_in(seeds[8], 71), 0)
    value_matrix = normal_values(seeds[5], (MODEL_WIDTH, KEY_VALUE_HEADS * HEAD_SIZE), MODEL_WIDTH ** -0.5, 0.09375, ((0, 8), (1, 4)))
    w_out = normal_values(seeds[6], (QUERY_HEADS * HEAD_SIZE, MODEL_WIDTH), (QUERY_HEADS * HEAD_SIZE) ** -0.5, 0.125, ((0, 4), (1, 8)))
    block_order = jax.random.permutation(seeds[7], 2 * N_CTX).astype(jnp.int32)
    return {"hidden": hidden, "target": target, "gain": gain, "w_query": w_query, "w_key": w_key, "value_matrix": value_matrix, "w_out": w_out, "block_order": block_order}


rope_base = 500000.0

def apply_rotary(values, token_places):
    half = values.shape[-1] // 2
    freqs = rope_base ** (-(jnp.arange(half, dtype=jnp.float32) * 2.0) / values.shape[-1])
    angles = token_places.astype(jnp.float32)[:, None] * freqs[None, :]
    cosine = jnp.cos(angles)[:, None, :]
    sine = jnp.sin(angles)[:, None, :]
    first = values[..., :half]
    second = values[..., half:]
    return jnp.concatenate([first * cosine - second * sine, second * cosine + first * sine], axis=-1)

def one_sequence(states, gain, w_query, w_key, value_matrix, w_out, token_places):
    query_group = QUERY_HEADS // KEY_VALUE_HEADS
    wide = states.astype(jnp.float32)
    normed = (wide * lax.rsqrt(lax.optimization_barrier(jnp.mean(wide * wide, axis=1, keepdims=True)) + 1e-05) * gain[None, :]).astype(jnp.bfloat16)
    query_rows = jnp.dot(normed, w_query, preferred_element_type=jnp.float32)
    key = jnp.dot(normed, w_key, preferred_element_type=jnp.float32)
    value_rows = jnp.dot(normed, value_matrix, preferred_element_type=jnp.float32)
    query_rows = apply_rotary(query_rows.reshape(SEQUENCE_LENGTH, QUERY_HEADS, HEAD_SIZE), token_places).astype(jnp.bfloat16).reshape(SEQUENCE_LENGTH, KEY_VALUE_HEADS, query_group, HEAD_SIZE)
    key = apply_rotary(key.reshape(SEQUENCE_LENGTH, KEY_VALUE_HEADS, HEAD_SIZE), token_places).astype(jnp.bfloat16)
    value_rows = value_rows.astype(jnp.bfloat16).reshape(SEQUENCE_LENGTH, KEY_VALUE_HEADS, HEAD_SIZE)
    scale = 1.0 / HEAD_SIZE ** 0.5
    block_rows = math.gcd(SEQUENCE_LENGTH, 1024)

    def head_split(index):
        qhead = lax.dynamic_index_in_dim(query_rows, index, 1, False)
        khead = lax.dynamic_index_in_dim(key, index, 1, False).astype(jnp.float32)
        vhead = lax.dynamic_index_in_dim(value_rows, index, 1, False).astype(jnp.float32)

        def per_block(number):
            first_row = (number * block_rows).astype(jnp.int32)
            qpart = lax.dynamic_slice_in_dim(qhead, first_row, block_rows, 0).astype(jnp.float32)
            qplaces = lax.dynamic_slice_in_dim(token_places, first_row, block_rows, 0)
            allowed = qplaces[:, None] >= token_places[None, :]
            scores = jnp.einsum('qgd,kd->gqk', qpart, khead) * scale
            scores = jnp.where(allowed[None], scores, -1e+30)
            peak = lax.optimization_barrier(jnp.max(scores, axis=-1, keepdims=True))
            weights = jnp.where(allowed[None], jnp.exp(scores - peak), 0.0)
            total = lax.optimization_barrier(jnp.sum(weights, axis=-1))
            rounded = weights.astype(jnp.bfloat16).astype(jnp.float32)
            mixed = jnp.einsum('gqk,kd->qgd', rounded, vhead)
            return (mixed / jnp.transpose(total)[:, :, None]).astype(jnp.bfloat16)
        pieces = lax.map(per_block, jnp.arange(SEQUENCE_LENGTH // block_rows, dtype=jnp.int32))
        return pieces.reshape(SEQUENCE_LENGTH, query_group, HEAD_SIZE)
    head_list = lax.map(head_split, jnp.arange(KEY_VALUE_HEADS, dtype=jnp.int32))
    attn = jnp.transpose(head_list, (1, 0, 2, 3)).reshape(SEQUENCE_LENGTH, QUERY_HEADS * HEAD_SIZE)
    width = QUERY_HEADS * HEAD_SIZE // N_TP
    summed = jnp.zeros((SEQUENCE_LENGTH, MODEL_WIDTH), jnp.float32)
    for part in range(N_TP):
        partial_term = jnp.dot(attn[:, part * width:(part + 1) * width], w_out[part * width:(part + 1) * width], preferred_element_type=jnp.float32)
        summed = summed + partial_term.astype(jnp.bfloat16).astype(jnp.float32)
    return summed.astype(jnp.bfloat16)

def reference(hidden, target, gain, w_query, w_key, value_matrix, w_out, block_order):
    rows = jnp.arange(SEQUENCE_LENGTH, dtype=jnp.int32)
    token_places = (jnp.take(block_order, rows // CH).astype(jnp.int32) * CH + rows % CH).astype(jnp.int32)
    outputs = []
    squares = jnp.zeros((), jnp.float32)
    for index in range(SEQS):
        result = one_sequence(hidden[index], gain, w_query, w_key, value_matrix, w_out, token_places)
        outputs.append(result)
        resid = hidden[index].astype(jnp.float32) + result.astype(jnp.float32) - target[index].astype(jnp.float32)
        squares = squares + jnp.sum(resid * resid)
    loss = squares / (SEQS * SEQUENCE_LENGTH * MODEL_WIDTH)
    return (jnp.stack(outputs), loss)
```

```python
import functools

import jax
import jax.numpy as jnp
from jax import lax
from jax.experimental import pallas as pl
from jax.experimental.pallas import tpu as pltpu
from jax.sharding import PartitionSpec as P

MODEL_WIDTH = 4096
QUERY_HEADS = 16
KEY_VALUE_HEADS = 4
HEAD_SIZE = 128


rope_base = 500000.0


def shifted(value, axis, by):
    peers = lax.axis_size(axis)
    return lax.ppermute(value, axis, [(i, (i + by) % peers) for i in range(peers)])


def positions(order, start, rows, half):
    index = start + lax.iota(jnp.int32, rows)
    block = index // half
    slots = lax.iota(jnp.int32, order.shape[0])
    chosen = jnp.sum(jnp.where(block[:, None] == slots[None, :], order[None, :], 0), axis=1)
    return chosen * half + index % half


def apply_rotary(values, token_places):
    half = values.shape[-1] // 2
    freqs = rope_base ** (-(jnp.arange(half, dtype=jnp.float32) * 2.0) / values.shape[-1])
    angles = token_places.astype(jnp.float32)[:, None] * freqs[None, :]
    cosine = jnp.cos(angles)[:, None, :]
    sine = jnp.sin(angles)[:, None, :]
    first = values[..., :half]
    second = values[..., half:]
    return jnp.concatenate(
        [first * cosine - second * sine, second * cosine + first * sine], axis=-1
    )


def attend(state, query_rows, qpos, piece, kpos):
    peak, total, accum = state
    rows = piece.shape[1]
    local_heads = query_rows.shape[1]
    pair = piece.reshape(2, rows, local_heads, HEAD_SIZE)
    scores = jnp.einsum(
        "qcgd,kcd->cgqk", query_rows, pair[0], preferred_element_type=jnp.float32
    ) * (1.0 / HEAD_SIZE**0.5)
    allowed = (qpos[:, None] >= kpos[None, :])[None, None]
    scores = jnp.where(allowed, scores, -1e30)
    new_peak = jnp.maximum(peak, jnp.max(scores, axis=-1))
    weights = jnp.where(allowed, jnp.exp(scores - new_peak[..., None]), 0.0)
    factor = jnp.exp(peak - new_peak)
    total = total * factor + jnp.sum(weights, axis=-1)
    update = jnp.einsum(
        "cgqk,kcd->qcgd", weights.astype(jnp.bfloat16), pair[1], preferred_element_type=jnp.float32
    )
    accum = accum * jnp.transpose(factor, (2, 0, 1))[..., None] + update
    return (new_peak, total, accum)


def on_device(hidden, target, gain, w_query, w_key, value_matrix, w_out, block_order):
    rows = hidden.shape[1]
    half = rows // 2
    local = hidden[0]
    whole = lax.all_gather(local, "tp", axis=1, tiled=True)
    wide = whole.astype(jnp.float32)
    normed = (
        wide * lax.rsqrt(jnp.mean(wide * wide, axis=1, keepdims=True) + 1e-05) * gain[None, :]
    ).astype(jnp.bfloat16)
    pieces = (
        lax.all_gather(w_query, ("ctx", "dp"), axis=0, tiled=True),
        lax.all_gather(w_key, ("ctx", "dp"), axis=0, tiled=True),
        lax.all_gather(value_matrix, ("ctx", "dp"), axis=0, tiled=True),
    )
    query_rows, key, value_rows = tuple(
        (jnp.dot(normed, piece, preferred_element_type=jnp.float32) for piece in pieces)
    )
    shard = lax.axis_index("ctx")
    qpos = positions(block_order, shard * rows, rows, half)
    local_heads = w_key.shape[1] // HEAD_SIZE
    query_group = QUERY_HEADS // KEY_VALUE_HEADS
    query_rows = (
        apply_rotary(query_rows.reshape(rows, local_heads * query_group, HEAD_SIZE), qpos)
        .astype(jnp.bfloat16)
        .reshape(rows, local_heads, query_group, HEAD_SIZE)
    )
    key = (
        apply_rotary(key.reshape(rows, local_heads, HEAD_SIZE), qpos)
        .astype(jnp.bfloat16)
        .reshape(rows, local_heads * HEAD_SIZE)
    )
    pair = jnp.stack([key, value_rows.astype(jnp.bfloat16)])
    state = (
        jnp.full((local_heads, query_group, rows), -1e30, jnp.float32),
        jnp.zeros((local_heads, query_group, rows), jnp.float32),
        jnp.zeros((rows, local_heads, query_group, HEAD_SIZE), jnp.float32),
    )
    count = lax.axis_size("ctx")
    state = attend(state, query_rows, qpos, pair, qpos)

    def turn(step, carry):
        moved, inner = carry
        moved = shifted(moved, "ctx", 1)
        source = (shard - step) % count
        return (
            moved,
            attend(
                inner, query_rows, qpos, moved, positions(block_order, source * rows, rows, half)
            ),
        )

    moved_end, state = lax.fori_loop(1, count, turn, (pair, state))
    peak, total, accum = state
    attn = (
        (accum / jnp.transpose(total, (2, 0, 1))[..., None])
        .astype(jnp.bfloat16)
        .reshape(rows, local_heads * query_group * HEAD_SIZE)
    )
    terms = jnp.dot(
        attn,
        lax.all_gather(w_out, ("ctx", "dp"), axis=1, tiled=True),
        preferred_element_type=jnp.float32,
    )
    summed = lax.psum_scatter(terms.astype(jnp.bfloat16), "tp", scatter_dimension=1, tiled=True)
    resid = local.astype(jnp.float32) + summed.astype(jnp.float32) - target[0].astype(jnp.float32)
    squares = lax.psum(jnp.sum(resid * resid), ("ctx", "tp", "dp"))
    loss = squares / (lax.axis_size("dp") * lax.axis_size("ctx") * rows * MODEL_WIDTH)
    return (summed[None], loss)


MESH = pl.DeviceIdType.MESH
F32 = jnp.float32
BF16 = jnp.bfloat16


def layer(
    nd,
    order,
    hidden,
    target,
    gain,
    freqs,
    w_query,
    w_key,
    value_matrix,
    w_out,
    out,
    loss,
    ga,
    go,
    xs,
    goal,
    normed,
    acc,
    trig,
    query,
    kv,
    attn,
    kept,
    sent,
    sib,
    ysend,
    yrecv,
    tile,
    sums_tp,
    sums_all,
    load_sem,
    a_send,
    a_recv,
    o_send,
    o_recv,
    h_send,
    h_recv,
    kv_send,
    kv_recv,
    s_send,
    s_recv,
    y_send,
    y_recv,
    t_send,
    t_recv,
    l_send,
    l_recv,
):
    c, t, d = lax.axis_index("ctx"), lax.axis_index("tp"), lax.axis_index("dp")
    nb = 2 * nd
    me = c * nd + d
    y, k = t // 2, t % 2
    sibling = y * 2 + (1 - k)
    across = (1 - y) * 2 + k
    diagonal = (1 - y) * 2 + (1 - k)
    rows, wide = hidden.shape
    deep = w_query.shape[0]
    qcols = w_query.shape[1]
    half = rows // 2
    n_heads = qcols // HEAD_SIZE
    e = d + 1 - 2 * (d % 2)

    loads = [
        pltpu.make_async_copy(w_query, ga.at[me, :, pl.ds(0, qcols)], load_sem.at[0]),
        pltpu.make_async_copy(w_key, ga.at[me, :, pl.ds(qcols, HEAD_SIZE)], load_sem.at[1]),
        pltpu.make_async_copy(
            value_matrix, ga.at[me, :, pl.ds(qcols + HEAD_SIZE, HEAD_SIZE)], load_sem.at[2]
        ),
        pltpu.make_async_copy(hidden, xs.at[t], load_sem.at[3]),
        pltpu.make_async_copy(w_out, go.at[me], load_sem.at[4]),
        pltpu.make_async_copy(target, goal, load_sem.at[5]),
    ]
    for load in loads:
        load.start()

    barrier = pltpu.get_barrier_semaphore()
    for s in range(1, nb):
        p = (me + s) % nb
        pl.semaphore_signal(
            barrier, inc=1, device_id={"ctx": p // nd, "dp": p % nd}, device_id_type=MESH
        )
    for s in (sibling, across, diagonal):
        pl.semaphore_signal(barrier, inc=1, device_id={"tp": s}, device_id_type=MESH)
    pl.semaphore_wait(barrier, nb + 2)

    def remote(src, dst, ssem, rsem, where):
        return pltpu.make_async_remote_copy(
            src_ref=src, dst_ref=dst, send_sem=ssem, recv_sem=rsem,
            device_id=where, device_id_type=MESH,
        )

    X, UP, DOWN = 0, 1, 2

    def piece(buf, ssem, rsem, b, way):
        where = {
            X: {"ctx": 1 - c},
            UP: {"dp": jnp.minimum(d + 1, nd - 1)},
            DOWN: {"dp": jnp.maximum(d - 1, 0)},
        }[way]
        return remote(buf.at[b], buf.at[b], ssem.at[way, b], rsem.at[b], where)

    def a_piece(b, way):
        return piece(ga, a_send, a_recv, b, way)

    def o_piece(b, way):
        return piece(go, o_send, o_recv, b, way)

    def block(src, j, dst, i, ssem, rsem, where):
        return remote(src.at[j], dst.at[i], ssem, rsem, {"tp": where})

    def h_copy(slot, i, where):
        return block(xs, slot, xs, slot, h_send.at[i], h_recv.at[i], where)

    h_sib = h_copy(t, 0, sibling)
    h_across = h_copy(t, 1, across)
    h_relay = h_copy(across, 2, sibling)
    for i in range(3):
        loads[i].wait()
    a_piece(me, X).start()
    up, down = d < nd - 1, d > 0

    @pl.when(up)
    def _():
        a_piece(me, UP).start()

    @pl.when(down)
    def _():
        a_piece(me, DOWN).start()

    loads[3].wait()
    h_across.start()
    h_sib.start()
    loads[4].wait()
    loads[5].wait()

    def positions_of(shard, index):
        low = order[2 * shard] * half
        high = order[2 * shard + 1] * half
        return jnp.where(index < half, low + index, high + index - half)

    place = positions_of(c, lax.broadcasted_iota(jnp.int32, (rows, HEAD_SIZE), 0)).astype(F32)
    angle = place * freqs[...]
    lane = lax.broadcasted_iota(jnp.int32, (rows, HEAD_SIZE), 1)
    trig[0] = jnp.cos(angle)
    sine = jnp.sin(angle)
    trig[1] = jnp.where(lane < HEAD_SIZE // 2, -sine, sine)

    def relay_a(s):
        @pl.when(d >= s)
        def _():
            b = me - s
            a_piece(b, DOWN).wait_recv()
            a_piece(b, X).start()

            @pl.when(up)
            def _():
                a_piece(b, UP).start()

        @pl.when(d + s < nd)
        def _():
            b = me + s
            a_piece(b, UP).wait_recv()
            a_piece(b, X).start()

            @pl.when(down)
            def _():
                a_piece(b, DOWN).start()

    relay_a(1)

    h_copy(across, 1, across).wait_recv()
    h_relay.start()
    h_copy(sibling, 0, sibling).wait_recv()
    h_copy(diagonal, 2, sibling).wait_recv()
    tp = xs.shape[0]
    chunk = 64
    per = wide // deep

    def norm_rows(i, carry):
        r = pl.multiple_of(i * chunk, chunk)
        total = jnp.zeros((chunk, 1), F32)
        for j in range(tp):
            v = xs[j, pl.ds(r, chunk), :].astype(F32)
            total = total + jnp.sum(v * v, axis=1, keepdims=True)
        scale = lax.rsqrt(total * (1.0 / (tp * wide)) + 1e-05)
        for j in range(tp):
            for m in range(per):
                v = xs[j, pl.ds(r, chunk), m * deep : (m + 1) * deep].astype(F32)
                g = gain[:, j * wide + m * deep : j * wide + (m + 1) * deep]
                normed[j * per + m, pl.ds(r, chunk), :] = (v * scale * g).astype(BF16)
        return carry

    lax.fori_loop(0, rows // chunk, norm_rows, 0)

    for s in range(2, nd):
        relay_a(s)
        if s == nd - 2:

            @pl.when(up)
            def _():
                o_piece(me, UP).start()

            @pl.when(down)
            def _():
                o_piece(me, DOWN).start()

    o_piece(me, X).start()
    acc[...] = jnp.zeros_like(acc)

    def project(b):
        acc[...] += jnp.dot(normed[b], ga[b], preferred_element_type=F32)

    def own_line(i, carry):
        project(c * nd + i)
        return carry

    lax.fori_loop(0, nd, own_line, 0)

    def relay_o_line(s):
        @pl.when(d >= s)
        def _():
            b = me - s
            o_piece(b, DOWN).wait_recv()

            @pl.when(up)
            def _():
                o_piece(b, UP).start()

        @pl.when(d + s < nd)
        def _():
            b = me + s
            o_piece(b, UP).wait_recv()

            @pl.when(down)
            def _():
                o_piece(b, DOWN).start()

    def relay_o_x(s):
        @pl.when((d >= s) & (d - s != e))
        def _():
            o_piece(me - s, X).start()

        @pl.when((d + s < nd) & (d + s != e))
        def _():
            o_piece(me + s, X).start()

    relay_o_line(1)

    def other_line(i, carry):
        far = jnp.where(d < nd // 2, i, nd - 1 - i)
        b = (1 - c) * nd + far
        a_piece(b, X).wait_recv()
        project(b)
        return carry

    lax.fori_loop(0, nd, other_line, 0)

    def rotated(v):
        return (v * trig[0] + pltpu.roll(v, HEAD_SIZE // 2, 1) * trig[1]).astype(BF16)

    kv[c, :, 0:HEAD_SIZE] = rotated(acc[:, qcols : qcols + HEAD_SIZE])
    kv[c, :, HEAD_SIZE:] = acc[:, qcols + HEAD_SIZE :].astype(BF16)
    kv_copy = remote(kv.at[c], kv.at[c], kv_send.at[0], kv_recv.at[0], {"ctx": 1 - c})
    kv_copy.start()
    relay_o_x(1)
    for h in range(n_heads):
        part = slice(h * HEAD_SIZE, (h + 1) * HEAD_SIZE)
        query[h] = rotated(acc[:, part])
    for s in range(2, nd):
        relay_o_line(s)
        relay_o_x(s)

    mirror = (1 - c) * nd + d
    o_piece(mirror, X).wait_recv()

    @pl.when(d % 2 == 0)
    def _():
        o_piece(mirror, UP).start()

    @pl.when(d % 2 == 1)
    def _():
        o_piece(mirror, DOWN).start()

    remote(kv.at[1 - c], kv.at[1 - c], kv_send.at[0], kv_recv.at[0], {"ctx": 1 - c}).wait_recv()
    qrows = 256
    dims = (((1,), (1,)), ((), ()))

    def attend_block(i, carry):
        h = i // (rows // qrows)
        r = pl.multiple_of((i % (rows // qrows)) * qrows, qrows)
        q = query[h, pl.ds(r, qrows), :]
        qpos = positions_of(c, r + lax.broadcasted_iota(jnp.int32, (qrows, rows), 0))
        scores = []
        for n in range(2):
            kpos = positions_of(n, lax.broadcasted_iota(jnp.int32, (qrows, rows), 1))
            sc = lax.dot_general(
                q, kv[n, :, 0:HEAD_SIZE], dims, preferred_element_type=F32
            ) * (1.0 / HEAD_SIZE**0.5)
            scores.append(jnp.where(qpos >= kpos, sc, -1e30))
        peak = jnp.maximum(
            jnp.max(scores[0], axis=1, keepdims=True), jnp.max(scores[1], axis=1, keepdims=True)
        )
        total = jnp.zeros((qrows, 1), F32)
        value = jnp.zeros((qrows, HEAD_SIZE), F32)
        for n in range(2):
            p = jnp.exp(scores[n] - peak)
            total = total + jnp.sum(p, axis=1, keepdims=True)
            value = value + jnp.dot(
                p.astype(BF16), kv[n, :, HEAD_SIZE:], preferred_element_type=F32
            )
        attn[h, pl.ds(r, qrows), :] = (value / total).astype(BF16)
        return carry

    lax.fori_loop(0, n_heads * (rows // qrows), attend_block, 0)

    js = nd // 2

    def out_block(b):
        full = jnp.concatenate([attn[h] for h in range(n_heads)], axis=1)
        return jnp.dot(full, go[b], preferred_element_type=F32).astype(BF16)

    def s_copy(side, j):
        i = side * js + j
        return block(sent, i, sib, i, s_send.at[i], s_recv.at[i], sibling)

    def y_copy(j):
        return block(ysend, j, yrecv, j, y_send.at[j], y_recv.at[j], across)

    for phase in range(2):
        side = c if phase == 0 else 1 - c

        def ready(within):
            if phase == 0:
                return

            @pl.when(within != d)
            def _():
                o_piece(side * nd + within, X).wait_recv()

        def give(j, carry):
            within = (1 - k) * js + j
            ready(within)
            sent[side * js + j] = out_block(side * nd + within)
            s_copy(side, j).start()
            return carry

        def keep(j, carry):
            within = k * js + j
            ready(within)
            kept[side * js + j] = out_block(side * nd + within)
            s_copy(side, j).wait_recv()

            @pl.when(side != y)
            def _():
                i = side * js + j
                ysend[j] = (kept[i].astype(F32) + sib[i].astype(F32)).astype(BF16)
                y_copy(j).start()

            return carry

        lax.fori_loop(0, js, give, 0)
        lax.fori_loop(0, js, keep, 0)

    cols = w_out.shape[1]
    tile[...] = jnp.zeros_like(tile)
    for j in range(js):
        y_copy(j).wait_recv()

        def finish(i, carry):
            r = pl.multiple_of(i * chunk, chunk)
            here = (pl.ds(r, chunk), slice(j * cols, (j + 1) * cols))
            mine = y * js + j
            rr = pl.ds(r, chunk)
            total = (
                kept[mine, rr, :].astype(F32) + sib[mine, rr, :].astype(F32)
            ) + yrecv[j, rr, :].astype(F32)
            result = total.astype(BF16)
            out[here] = result
            resid = xs[t, rr, j * cols : (j + 1) * cols].astype(F32) + result.astype(F32)
            resid = resid - goal[rr, j * cols : (j + 1) * cols].astype(F32)
            sq = jnp.sum((resid * resid).reshape(chunk // 8, 8, cols), axis=0)
            part = sq[:, 0:128]
            for m in range(1, cols // 128):
                part = part + sq[:, m * 128 : (m + 1) * 128]
            tile[...] += part
            return carry

        lax.fori_loop(0, rows // chunk, finish, 0)

    sums_tp[0] = tile[...]
    tp_copies = [
        block(sums_tp, 0, sums_tp, 1 + i, t_send.at[i], t_recv.at[i], where)
        for i, where in enumerate((sibling, across, diagonal))
    ]
    for copy in tp_copies:
        copy.start()
    for copy in tp_copies:
        copy.wait_recv()
    sums_all[me] = (sums_tp[0] + sums_tp[1]) + (sums_tp[2] + sums_tp[3])

    def l_copy(s, slot):
        p = (me + s) % nb
        return remote(
            sums_all.at[slot], sums_all.at[slot], l_send.at[s], l_recv.at[slot],
            {"ctx": p // nd, "dp": p % nd},
        )

    for s in range(1, nb):
        l_copy(s, me).start()
    for s in range(1, nb):
        l_copy(s, (me + s) % nb).wait_recv()
    whole = sums_all[0]
    for b in range(1, nb):
        whole = whole + sums_all[b]
    count = tp * wide * rows * nb
    loss[...] = jnp.full(loss.shape, jnp.sum(whole) / count, F32)

    h_across.wait_send()
    h_sib.wait_send()
    h_relay.wait_send()
    kv_copy.wait_send()
    for copy in tp_copies:
        copy.wait_send()
    for s in range(1, nb):
        l_copy(s, me).wait_send()
    for side in range(2):
        for j in range(js):
            s_copy(side, j).wait_send()
    for j in range(js):
        y_copy(j).wait_send()
    a_piece(me, X).wait_send()
    o_piece(me, X).wait_send()
    for s in range(0, nd):
        for sign in (-1, 1) if s else (1,):
            b = me + sign * s
            there = (d + sign * s >= 0) & (d + sign * s < nd)
            if s:

                @pl.when(there)
                def _():
                    a_piece(b, X).wait_send()

                @pl.when(there & (d + sign * s != e))
                def _():
                    o_piece(b, X).wait_send()

            if s == 0 or sign < 0:

                @pl.when(there & up)
                def _():
                    a_piece(b, UP).wait_send()
                    o_piece(b, UP).wait_send()

            if s == 0 or sign > 0:

                @pl.when(there & down)
                def _():
                    a_piece(b, DOWN).wait_send()
                    o_piece(b, DOWN).wait_send()

    @pl.when(d % 2 == 0)
    def _():
        o_piece(mirror, UP).wait_send()

    @pl.when(d % 2 == 1)
    def _():
        o_piece(mirror, DOWN).wait_send()


def fused(nd, hidden, target, gain, w_query, w_key, value_matrix, w_out, block_order):
    rows, wide = hidden.shape[1:]
    nb = 2 * nd
    tp = lax.axis_size("tp")
    deep, qcols = w_query.shape
    all_cols = qcols + w_key.shape[1] + value_matrix.shape[1]
    orows, ocols = w_out.shape
    half = HEAD_SIZE // 2
    freqs = rope_base ** (-(jnp.arange(half, dtype=F32) * 2.0) / HEAD_SIZE)
    freqs = jnp.concatenate([freqs, freqs])[None, :]
    heads = qcols // HEAD_SIZE
    js = nd // 2
    vmem = pl.BlockSpec(memory_space=pltpu.VMEM)
    anyspace = pl.BlockSpec(memory_space=pl.ANY)
    dma = pltpu.SemaphoreType.DMA
    branch, loss = pl.pallas_call(
        functools.partial(layer, nd),
        out_shape=(
            jax.ShapeDtypeStruct((rows, wide), BF16),
            jax.ShapeDtypeStruct((8, 128), F32),
        ),
        in_specs=[
            pl.BlockSpec(memory_space=pltpu.SMEM),
            anyspace,
            anyspace,
            vmem,
            vmem,
            anyspace,
            anyspace,
            anyspace,
            anyspace,
        ],
        out_specs=(vmem, vmem),
        scratch_shapes=[
            pltpu.VMEM((nb, deep, all_cols), BF16),
            pltpu.VMEM((nb, orows, ocols), BF16),
            pltpu.VMEM((tp, rows, wide), BF16),
            pltpu.VMEM((rows, wide), BF16),
            pltpu.VMEM((nb, rows, deep), BF16),
            pltpu.VMEM((rows, all_cols), F32),
            pltpu.VMEM((2, rows, HEAD_SIZE), F32),
            pltpu.VMEM((heads, rows, HEAD_SIZE), BF16),
            pltpu.VMEM((2, rows, 2 * HEAD_SIZE), BF16),
            pltpu.VMEM((heads, rows, HEAD_SIZE), BF16),
            pltpu.VMEM((2 * js, rows, ocols), BF16),
            pltpu.VMEM((2 * js, rows, ocols), BF16),
            pltpu.VMEM((2 * js, rows, ocols), BF16),
            pltpu.VMEM((js, rows, ocols), BF16),
            pltpu.VMEM((js, rows, ocols), BF16),
            pltpu.VMEM((8, 128), F32),
            pltpu.VMEM((tp, 8, 128), F32),
            pltpu.VMEM((nb, 8, 128), F32),
            dma((6,)),
            dma((3, nb)),
            dma((nb,)),
            dma((3, nb)),
            dma((nb,)),
            dma((3,)),
            dma((3,)),
            dma((1,)),
            dma((1,)),
            dma((2 * js,)),
            dma((2 * js,)),
            dma((js,)),
            dma((js,)),
            dma((3,)),
            dma((3,)),
            dma((nb,)),
            dma((nb,)),
        ],
        compiler_params=pltpu.CompilerParams(
            collective_id=1, has_side_effects=True, vmem_limit_bytes=60 * 1024 * 1024
        ),
    )(
        block_order,
        hidden[0],
        target[0],
        gain[None, :],
        freqs,
        w_query,
        w_key,
        value_matrix,
        w_out,
    )
    return (branch[None], loss[0, 0])


def solution(mesh):
    in_specs = (
        P("dp", "ctx", "tp"),
        P("dp", "ctx", "tp"),
        P(),
        P(("ctx", "dp"), "tp"),
        P(("ctx", "dp"), "tp"),
        P(("ctx", "dp"), "tp"),
        P("tp", ("ctx", "dp")),
        P(),
    )
    out_specs = (P("dp", "ctx", "tp"), P())
    sizes = mesh.shape
    fits = sizes["ctx"] == 2 and sizes["tp"] == 4 and sizes["dp"] % 2 == 0
    body = functools.partial(fused, sizes["dp"]) if fits else on_device
    return jax.shard_map(
        body, mesh=mesh, in_specs=in_specs, out_specs=out_specs, check_vma=False
    )
```

```python
import functools

import jax
import jax.numpy as jnp
from jax import lax
from jax.experimental import pallas as pl
from jax.experimental.pallas import tpu as pltpu
from jax.sharding import PartitionSpec as P

MODEL_WIDTH = 4096
QUERY_HEADS = 16
KEY_VALUE_HEADS = 4
HEAD_SIZE = 128


rope_base = 500000.0


def shifted(value, axis, by):
    peers = lax.axis_size(axis)
    return lax.ppermute(value, axis, [(i, (i + by) % peers) for i in range(peers)])


def positions(order, start, rows, half):
    index = start + lax.iota(jnp.int32, rows)
    block = index // half
    slots = lax.iota(jnp.int32, order.shape[0])
    chosen = jnp.sum(jnp.where(block[:, None] == slots[None, :], order[None, :], 0), axis=1)
    return chosen * half + index % half


def apply_rotary(values, token_places):
    half = values.shape[-1] // 2
    freqs = rope_base ** (-(jnp.arange(half, dtype=jnp.float32) * 2.0) / values.shape[-1])
    angles = token_places.astype(jnp.float32)[:, None] * freqs[None, :]
    cosine = jnp.cos(angles)[:, None, :]
    sine = jnp.sin(angles)[:, None, :]
    first = values[..., :half]
    second = values[..., half:]
    return jnp.concatenate(
        [first * cosine - second * sine, second * cosine + first * sine], axis=-1
    )


def attend(state, query_rows, qpos, piece, kpos):
    peak, total, accum = state
    rows = piece.shape[1]
    local_heads = query_rows.shape[1]
    pair = piece.reshape(2, rows, local_heads, HEAD_SIZE)
    scores = jnp.einsum(
        "qcgd,kcd->cgqk", query_rows, pair[0], preferred_element_type=jnp.float32
    ) * (1.0 / HEAD_SIZE**0.5)
    allowed = (qpos[:, None] >= kpos[None, :])[None, None]
    scores = jnp.where(allowed, scores, -1e30)
    new_peak = jnp.maximum(peak, jnp.max(scores, axis=-1))
    weights = jnp.where(allowed, jnp.exp(scores - new_peak[..., None]), 0.0)
    factor = jnp.exp(peak - new_peak)
    total = total * factor + jnp.sum(weights, axis=-1)
    update = jnp.einsum(
        "cgqk,kcd->qcgd", weights.astype(jnp.bfloat16), pair[1], preferred_element_type=jnp.float32
    )
    accum = accum * jnp.transpose(factor, (2, 0, 1))[..., None] + update
    return (new_peak, total, accum)


def on_device(hidden, target, gain, w_query, w_key, value_matrix, w_out, block_order):
    rows = hidden.shape[1]
    half = rows // 2
    local = hidden[0]
    whole = lax.all_gather(local, "tp", axis=1, tiled=True)
    wide = whole.astype(jnp.float32)
    normed = (
        wide * lax.rsqrt(jnp.mean(wide * wide, axis=1, keepdims=True) + 1e-05) * gain[None, :]
    ).astype(jnp.bfloat16)
    pieces = (
        lax.all_gather(w_query, ("ctx", "dp"), axis=0, tiled=True),
        lax.all_gather(w_key, ("ctx", "dp"), axis=0, tiled=True),
        lax.all_gather(value_matrix, ("ctx", "dp"), axis=0, tiled=True),
    )
    query_rows, key, value_rows = tuple(
        (jnp.dot(normed, piece, preferred_element_type=jnp.float32) for piece in pieces)
    )
    shard = lax.axis_index("ctx")
    qpos = positions(block_order, shard * rows, rows, half)
    local_heads = w_key.shape[1] // HEAD_SIZE
    query_group = QUERY_HEADS // KEY_VALUE_HEADS
    query_rows = (
        apply_rotary(query_rows.reshape(rows, local_heads * query_group, HEAD_SIZE), qpos)
        .astype(jnp.bfloat16)
        .reshape(rows, local_heads, query_group, HEAD_SIZE)
    )
    key = (
        apply_rotary(key.reshape(rows, local_heads, HEAD_SIZE), qpos)
        .astype(jnp.bfloat16)
        .reshape(rows, local_heads * HEAD_SIZE)
    )
    pair = jnp.stack([key, value_rows.astype(jnp.bfloat16)])
    state = (
        jnp.full((local_heads, query_group, rows), -1e30, jnp.float32),
        jnp.zeros((local_heads, query_group, rows), jnp.float32),
        jnp.zeros((rows, local_heads, query_group, HEAD_SIZE), jnp.float32),
    )
    count = lax.axis_size("ctx")
    state = attend(state, query_rows, qpos, pair, qpos)

    def turn(step, carry):
        moved, inner = carry
        moved = shifted(moved, "ctx", 1)
        source = (shard - step) % count
        return (
            moved,
            attend(
                inner, query_rows, qpos, moved, positions(block_order, source * rows, rows, half)
            ),
        )

    moved_end, state = lax.fori_loop(1, count, turn, (pair, state))
    peak, total, accum = state
    attn = (
        (accum / jnp.transpose(total, (2, 0, 1))[..., None])
        .astype(jnp.bfloat16)
        .reshape(rows, local_heads * query_group * HEAD_SIZE)
    )
    terms = jnp.dot(
        attn,
        lax.all_gather(w_out, ("ctx", "dp"), axis=1, tiled=True),
        preferred_element_type=jnp.float32,
    )
    summed = lax.psum_scatter(terms.astype(jnp.bfloat16), "tp", scatter_dimension=1, tiled=True)
    resid = local.astype(jnp.float32) + summed.astype(jnp.float32) - target[0].astype(jnp.float32)
    squares = lax.psum(jnp.sum(resid * resid), ("ctx", "tp", "dp"))
    loss = squares / (lax.axis_size("dp") * lax.axis_size("ctx") * rows * MODEL_WIDTH)
    return (summed[None], loss)


MESH = pl.DeviceIdType.MESH
F32 = jnp.float32
BF16 = jnp.bfloat16


def layer(
    nd,
    order,
    hidden,
    target,
    gain,
    freqs,
    w_query,
    w_key,
    value_matrix,
    w_out,
    out,
    loss,
    ga,
    go,
    xs,
    goal,
    normed,
    acc,
    trig,
    query,
    kv,
    attn,
    kept,
    sent,
    sib,
    ysend,
    yrecv,
    tile,
    sums_tp,
    sums_all,
    load_sem,
    a_send,
    a_recv,
    o_send,
    o_recv,
    h_send,
    h_recv,
    kv_send,
    kv_recv,
    s_send,
    s_recv,
    y_send,
    y_recv,
    t_send,
    t_recv,
    l_send,
    l_recv,
):
    c, t, d = lax.axis_index("ctx"), lax.axis_index("tp"), lax.axis_index("dp")
    nb = 2 * nd
    me = c * nd + d
    y, k = t // 2, t % 2
    sibling = y * 2 + (1 - k)
    across = (1 - y) * 2 + k
    diagonal = (1 - y) * 2 + (1 - k)
    rows, wide = hidden.shape
    deep = w_query.shape[0]
    qcols = w_query.shape[1]
    half = rows // 2
    n_heads = qcols // HEAD_SIZE
    e = d + 1 - 2 * (d % 2)

    loads = [
        pltpu.make_async_copy(w_query, ga.at[me, :, pl.ds(0, qcols)], load_sem.at[0]),
        pltpu.make_async_copy(w_key, ga.at[me, :, pl.ds(qcols, HEAD_SIZE)], load_sem.at[1]),
        pltpu.make_async_copy(
            value_matrix, ga.at[me, :, pl.ds(qcols + HEAD_SIZE, HEAD_SIZE)], load_sem.at[2]
        ),
        pltpu.make_async_copy(hidden, xs.at[t], load_sem.at[3]),
        pltpu.make_async_copy(w_out, go.at[me], load_sem.at[4]),
        pltpu.make_async_copy(target, goal, load_sem.at[5]),
    ]
    for load in loads:
        load.start()

    barrier = pltpu.get_barrier_semaphore()
    for s in range(1, nb):
        p = (me + s) % nb
        pl.semaphore_signal(
            barrier, inc=1, device_id={"ctx": p // nd, "dp": p % nd}, device_id_type=MESH
        )
    for s in (sibling, across, diagonal):
        pl.semaphore_signal(barrier, inc=1, device_id={"tp": s}, device_id_type=MESH)
    pl.semaphore_wait(barrier, nb + 2)

    def remote(src, dst, ssem, rsem, where):
        return pltpu.make_async_remote_copy(
            src_ref=src, dst_ref=dst, send_sem=ssem, recv_sem=rsem,
            device_id=where, device_id_type=MESH,
        )

    X, UP, DOWN = 0, 1, 2

    def piece(buf, ssem, rsem, b, way):
        where = {
            X: {"ctx": 1 - c},
            UP: {"dp": jnp.minimum(d + 1, nd - 1)},
            DOWN: {"dp": jnp.maximum(d - 1, 0)},
        }[way]
        return remote(buf.at[b], buf.at[b], ssem.at[way, b], rsem.at[b], where)

    def a_piece(b, way):
        return piece(ga, a_send, a_recv, b, way)

    def o_piece(b, way):
        return piece(go, o_send, o_recv, b, way)

    def block(src, j, dst, i, ssem, rsem, where):
        return remote(src.at[j], dst.at[i], ssem, rsem, {"tp": where})

    def h_copy(slot, i, where):
        return block(xs, slot, xs, slot, h_send.at[i], h_recv.at[i], where)

    h_sib = h_copy(t, 0, sibling)
    h_across = h_copy(t, 1, across)
    h_relay = h_copy(across, 2, sibling)
    for i in range(3):
        loads[i].wait()
    a_piece(me, X).start()
    up, down = d < nd - 1, d > 0

    @pl.when(up)
    def _():
        a_piece(me, UP).start()

    @pl.when(down)
    def _():
        a_piece(me, DOWN).start()

    loads[3].wait()
    h_across.start()
    h_sib.start()
    loads[4].wait()
    loads[5].wait()

    def positions_of(shard, index):
        low = order[2 * shard] * half
        high = order[2 * shard + 1] * half
        return jnp.where(index < half, low + index, high + index - half)

    place = positions_of(c, lax.broadcasted_iota(jnp.int32, (rows, HEAD_SIZE), 0)).astype(F32)
    angle = place * freqs[...]
    lane = lax.broadcasted_iota(jnp.int32, (rows, HEAD_SIZE), 1)
    trig[0] = jnp.cos(angle)
    sine = jnp.sin(angle)
    trig[1] = jnp.where(lane < HEAD_SIZE // 2, -sine, sine)

    def relay_a(s):
        @pl.when(d >= s)
        def _():
            b = me - s
            a_piece(b, DOWN).wait_recv()
            a_piece(b, X).start()

            @pl.when(up)
            def _():
                a_piece(b, UP).start()

        @pl.when(d + s < nd)
        def _():
            b = me + s
            a_piece(b, UP).wait_recv()
            a_piece(b, X).start()

            @pl.when(down)
            def _():
                a_piece(b, DOWN).start()

    relay_a(1)

    h_copy(across, 1, across).wait_recv()
    h_relay.start()
    h_copy(sibling, 0, sibling).wait_recv()
    h_copy(diagonal, 2, sibling).wait_recv()
    tp = xs.shape[0]
    chunk = 64
    per = wide // deep

    def norm_rows(i, carry):
        r = pl.multiple_of(i * chunk, chunk)
        total = jnp.zeros((chunk, 1), F32)
        for j in range(tp):
            v = xs[j, pl.ds(r, chunk), :].astype(F32)
            total = total + jnp.sum(v * v, axis=1, keepdims=True)
        scale = lax.rsqrt(total * (1.0 / (tp * wide)) + 1e-05)
        for j in range(tp):
            for m in range(per):
                v = xs[j, pl.ds(r, chunk), m * deep : (m + 1) * deep].astype(F32)
                g = gain[:, j * wide + m * deep : j * wide + (m + 1) * deep]
                normed[j * per + m, pl.ds(r, chunk), :] = (v * scale * g).astype(BF16)
        return carry

    lax.fori_loop(0, rows // chunk, norm_rows, 0)

    for s in range(2, nd):
        relay_a(s)
        if s == nd - 2:

            @pl.when(up)
            def _():
                o_piece(me, UP).start()

            @pl.when(down)
            def _():
                o_piece(me, DOWN).start()

    o_piece(me, X).start()
    acc[...] = jnp.zeros_like(acc)

    def project(b):
        acc[...] += jnp.dot(normed[b], ga[b], preferred_element_type=F32)

    def own_line(i, carry):
        project(c * nd + i)
        return carry

    lax.fori_loop(0, nd, own_line, 0)

    def relay_o_line(s):
        @pl.when(d >= s)
        def _():
            b = me - s
            o_piece(b, DOWN).wait_recv()

            @pl.when(up)
            def _():
                o_piece(b, UP).start()

        @pl.when(d + s < nd)
        def _():
            b = me + s
            o_piece(b, UP).wait_recv()

            @pl.when(down)
            def _():
                o_piece(b, DOWN).start()

    def relay_o_x(s):
        @pl.when((d >= s) & (d - s != e))
        def _():
            o_piece(me - s, X).start()

        @pl.when((d + s < nd) & (d + s != e))
        def _():
            o_piece(me + s, X).start()

    relay_o_line(1)

    def other_line(i, carry):
        far = jnp.where(d < nd // 2, i, nd - 1 - i)
        b = (1 - c) * nd + far
        a_piece(b, X).wait_recv()
        project(b)
        return carry

    lax.fori_loop(0, nd, other_line, 0)

    def rotated(v):
        return (v * trig[0] + pltpu.roll(v, HEAD_SIZE // 2, 1) * trig[1]).astype(BF16)

    kv[c, :, 0:HEAD_SIZE] = rotated(acc[:, qcols : qcols + HEAD_SIZE])
    kv[c, :, HEAD_SIZE:] = acc[:, qcols + HEAD_SIZE :].astype(BF16)
    kv_copy = remote(kv.at[c], kv.at[c], kv_send.at[0], kv_recv.at[0], {"ctx": 1 - c})
    kv_copy.start()
    relay_o_x(1)
    for h in range(n_heads):
        part = slice(h * HEAD_SIZE, (h + 1) * HEAD_SIZE)
        query[h] = rotated(acc[:, part])
    for s in range(2, nd):
        relay_o_line(s)
        relay_o_x(s)

    mirror = (1 - c) * nd + d
    o_piece(mirror, X).wait_recv()

    @pl.when(d % 2 == 0)
    def _():
        o_piece(mirror, UP).start()

    @pl.when(d % 2 == 1)
    def _():
        o_piece(mirror, DOWN).start()

    remote(kv.at[1 - c], kv.at[1 - c], kv_send.at[0], kv_recv.at[0], {"ctx": 1 - c}).wait_recv()
    qrows = 256
    dims = (((1,), (1,)), ((), ()))

    def attend_block(i, carry):
        h = i // (rows // qrows)
        r = pl.multiple_of((i % (rows // qrows)) * qrows, qrows)
        q = query[h, pl.ds(r, qrows), :]
        qpos = positions_of(c, r + lax.broadcasted_iota(jnp.int32, (qrows, rows), 0))
        scores = []
        for n in range(2):
            kpos = positions_of(n, lax.broadcasted_iota(jnp.int32, (qrows, rows), 1))
            sc = lax.dot_general(
                q, kv[n, :, 0:HEAD_SIZE], dims, preferred_element_type=F32
            ) * (1.0 / HEAD_SIZE**0.5)
            scores.append(jnp.where(qpos >= kpos, sc, -1e30))
        peak = jnp.maximum(
            jnp.max(scores[0], axis=1, keepdims=True), jnp.max(scores[1], axis=1, keepdims=True)
        )
        total = jnp.zeros((qrows, 1), F32)
        value = jnp.zeros((qrows, HEAD_SIZE), F32)
        for n in range(2):
            p = jnp.exp(scores[n] - peak)
            total = total + jnp.sum(p, axis=1, keepdims=True)
            value = value + jnp.dot(
                p.astype(BF16), kv[n, :, HEAD_SIZE:], preferred_element_type=F32
            )
        attn[h, pl.ds(r, qrows), :] = (value / total).astype(BF16)
        return carry

    lax.fori_loop(0, n_heads * (rows // qrows), attend_block, 0)

    js = nd // 2

    def out_block(b):
        full = jnp.concatenate([attn[h] for h in range(n_heads)], axis=1)
        return jnp.dot(full, go[b], preferred_element_type=F32).astype(BF16)

    def s_copy(side, j):
        i = side * js + j
        return block(sent, i, sib, i, s_send.at[i], s_recv.at[i], sibling)

    def y_copy(j):
        return block(ysend, j, yrecv, j, y_send.at[j], y_recv.at[j], across)

    near = d < js

    def arrival(i):
        pair, r = i // 2, i % 2
        group = (d // 2 + pair) % js
        mine = jnp.where(r == 0, d, e)
        return jnp.where(pair == 0, mine, group * 2 + jnp.where(near, r, 1 - r))

    for phase in range(2):
        side = c if phase == 0 else 1 - c

        def columns(i, carry):
            within = arrival(i)
            if phase == 1:

                @pl.when(within != d)
                def _():
                    o_piece(side * nd + within, X).wait_recv()

            j = within % js
            slot = side * js + j
            value = out_block(side * nd + within)
            own = within // js == k

            @pl.when(jnp.logical_not(own))
            def _():
                sent[slot] = value
                s_copy(side, j).start()

            @pl.when(own)
            def _():
                kept[slot] = value
                s_copy(side, j).wait_recv()

                @pl.when(side != y)
                def _():
                    ysend[j] = (kept[slot].astype(F32) + sib[slot].astype(F32)).astype(BF16)
                    y_copy(j).start()

            return carry

        lax.fori_loop(0, nd, columns, 0)

    cols = w_out.shape[1]
    tile[...] = jnp.zeros_like(tile)
    def finish_block(n, carry):
        j = jnp.where(near, n, js - 1 - n)
        y_copy(j).wait_recv()
        place = pl.ds(pl.multiple_of(j * cols, cols), cols)
        mine = y * js + j

        def finish(i, inner):
            rr = pl.ds(pl.multiple_of(i * chunk, chunk), chunk)
            total = (
                kept[mine, rr, :].astype(F32) + sib[mine, rr, :].astype(F32)
            ) + yrecv[j, rr, :].astype(F32)
            result = total.astype(BF16)
            out[rr, place] = result
            resid = xs[t, rr, place].astype(F32) + result.astype(F32)
            resid = resid - goal[rr, place].astype(F32)
            sq = jnp.sum((resid * resid).reshape(chunk // 8, 8, cols), axis=0)
            part = sq[:, 0:128]
            for m in range(1, cols // 128):
                part = part + sq[:, m * 128 : (m + 1) * 128]
            tile[...] += part
            return inner

        lax.fori_loop(0, rows // chunk, finish, 0)
        return carry

    lax.fori_loop(0, js, finish_block, 0)

    sums_tp[0] = tile[...]
    tp_copies = [
        block(sums_tp, 0, sums_tp, 1 + i, t_send.at[i], t_recv.at[i], where)
        for i, where in enumerate((sibling, across, diagonal))
    ]
    for copy in tp_copies:
        copy.start()
    for copy in tp_copies:
        copy.wait_recv()
    sums_all[me] = (sums_tp[0] + sums_tp[1]) + (sums_tp[2] + sums_tp[3])

    def l_copy(s, slot):
        p = (me + s) % nb
        return remote(
            sums_all.at[slot], sums_all.at[slot], l_send.at[s], l_recv.at[slot],
            {"ctx": p // nd, "dp": p % nd},
        )

    for s in range(1, nb):
        l_copy(s, me).start()
    for s in range(1, nb):
        l_copy(s, (me + s) % nb).wait_recv()
    whole = sums_all[0]
    for b in range(1, nb):
        whole = whole + sums_all[b]
    count = tp * wide * rows * nb
    loss[0, 0] = jnp.sum(whole) / count

    h_across.wait_send()
    h_sib.wait_send()
    h_relay.wait_send()
    kv_copy.wait_send()
    for copy in tp_copies:
        copy.wait_send()
    for s in range(1, nb):
        l_copy(s, me).wait_send()
    for side in range(2):
        for j in range(js):
            s_copy(side, j).wait_send()
    for j in range(js):
        y_copy(j).wait_send()
    a_piece(me, X).wait_send()
    o_piece(me, X).wait_send()
    for s in range(0, nd):
        for sign in (-1, 1) if s else (1,):
            b = me + sign * s
            there = (d + sign * s >= 0) & (d + sign * s < nd)
            if s:

                @pl.when(there)
                def _():
                    a_piece(b, X).wait_send()

                @pl.when(there & (d + sign * s != e))
                def _():
                    o_piece(b, X).wait_send()

            if s == 0 or sign < 0:

                @pl.when(there & up)
                def _():
                    a_piece(b, UP).wait_send()
                    o_piece(b, UP).wait_send()

            if s == 0 or sign > 0:

                @pl.when(there & down)
                def _():
                    a_piece(b, DOWN).wait_send()
                    o_piece(b, DOWN).wait_send()

    @pl.when(d % 2 == 0)
    def _():
        o_piece(mirror, UP).wait_send()

    @pl.when(d % 2 == 1)
    def _():
        o_piece(mirror, DOWN).wait_send()


def fused(nd, hidden, target, gain, w_query, w_key, value_matrix, w_out, block_order):
    rows, wide = hidden.shape[1:]
    nb = 2 * nd
    tp = lax.axis_size("tp")
    deep, qcols = w_query.shape
    all_cols = qcols + w_key.shape[1] + value_matrix.shape[1]
    orows, ocols = w_out.shape
    half = HEAD_SIZE // 2
    freqs = rope_base ** (-(jnp.arange(half, dtype=F32) * 2.0) / HEAD_SIZE)
    freqs = jnp.concatenate([freqs, freqs])[None, :]
    heads = qcols // HEAD_SIZE
    js = nd // 2
    vmem = pl.BlockSpec(memory_space=pltpu.VMEM)
    anyspace = pl.BlockSpec(memory_space=pl.ANY)
    dma = pltpu.SemaphoreType.DMA
    branch, loss = pl.pallas_call(
        functools.partial(layer, nd),
        out_shape=(
            jax.ShapeDtypeStruct((rows, wide), BF16),
            jax.ShapeDtypeStruct((1, 1), F32),
        ),
        in_specs=[
            pl.BlockSpec(memory_space=pltpu.SMEM),
            anyspace,
            anyspace,
            vmem,
            vmem,
            anyspace,
            anyspace,
            anyspace,
            anyspace,
        ],
        out_specs=(vmem, pl.BlockSpec(memory_space=pltpu.SMEM)),
        scratch_shapes=[
            pltpu.VMEM((nb, deep, all_cols), BF16),
            pltpu.VMEM((nb, orows, ocols), BF16),
            pltpu.VMEM((tp, rows, wide), BF16),
            pltpu.VMEM((rows, wide), BF16),
            pltpu.VMEM((nb, rows, deep), BF16),
            pltpu.VMEM((rows, all_cols), F32),
            pltpu.VMEM((2, rows, HEAD_SIZE), F32),
            pltpu.VMEM((heads, rows, HEAD_SIZE), BF16),
            pltpu.VMEM((2, rows, 2 * HEAD_SIZE), BF16),
            pltpu.VMEM((heads, rows, HEAD_SIZE), BF16),
            pltpu.VMEM((2 * js, rows, ocols), BF16),
            pltpu.VMEM((2 * js, rows, ocols), BF16),
            pltpu.VMEM((2 * js, rows, ocols), BF16),
            pltpu.VMEM((js, rows, ocols), BF16),
            pltpu.VMEM((js, rows, ocols), BF16),
            pltpu.VMEM((8, 128), F32),
            pltpu.VMEM((tp, 8, 128), F32),
            pltpu.VMEM((nb, 8, 128), F32),
            dma((6,)),
            dma((3, nb)),
            dma((nb,)),
            dma((3, nb)),
            dma((nb,)),
            dma((3,)),
            dma((3,)),
            dma((1,)),
            dma((1,)),
            dma((2 * js,)),
            dma((2 * js,)),
            dma((js,)),
            dma((js,)),
            dma((3,)),
            dma((3,)),
            dma((nb,)),
            dma((nb,)),
        ],
        compiler_params=pltpu.CompilerParams(
            collective_id=1, has_side_effects=True, vmem_limit_bytes=60 * 1024 * 1024
        ),
    )(
        block_order,
        hidden[0],
        target[0],
        gain[None, :],
        freqs,
        w_query,
        w_key,
        value_matrix,
        w_out,
    )
    return (branch[None], loss.reshape(()))


def solution(mesh):
    in_specs = (
        P("dp", "ctx", "tp"),
        P("dp", "ctx", "tp"),
        P(),
        P(("ctx", "dp"), "tp"),
        P(("ctx", "dp"), "tp"),
        P(("ctx", "dp"), "tp"),
        P("tp", ("ctx", "dp")),
        P(),
    )
    out_specs = (P("dp", "ctx", "tp"), P())
    sizes = mesh.shape
    fits = sizes["ctx"] == 2 and sizes["tp"] == 4 and sizes["dp"] % 2 == 0
    body = functools.partial(fused, sizes["dp"]) if fits else on_device
    return jax.shard_map(
        body, mesh=mesh, in_specs=in_specs, out_specs=out_specs, check_vma=False
    )
```

```python
import functools

import jax
import jax.numpy as jnp
from jax import lax
from jax.experimental import pallas as pl
from jax.experimental.pallas import tpu as pltpu
from jax.sharding import PartitionSpec as P

MODEL_WIDTH = 4096
QUERY_HEADS = 16
KEY_VALUE_HEADS = 4
HEAD_SIZE = 128


rope_base = 500000.0


def shifted(value, axis, by):
    peers = lax.axis_size(axis)
    return lax.ppermute(value, axis, [(i, (i + by) % peers) for i in range(peers)])


def positions(order, start, rows, half):
    index = start + lax.iota(jnp.int32, rows)
    block = index // half
    slots = lax.iota(jnp.int32, order.shape[0])
    chosen = jnp.sum(jnp.where(block[:, None] == slots[None, :], order[None, :], 0), axis=1)
    return chosen * half + index % half


def apply_rotary(values, token_places):
    half = values.shape[-1] // 2
    freqs = rope_base ** (-(jnp.arange(half, dtype=jnp.float32) * 2.0) / values.shape[-1])
    angles = token_places.astype(jnp.float32)[:, None] * freqs[None, :]
    cosine = jnp.cos(angles)[:, None, :]
    sine = jnp.sin(angles)[:, None, :]
    first = values[..., :half]
    second = values[..., half:]
    return jnp.concatenate(
        [first * cosine - second * sine, second * cosine + first * sine], axis=-1
    )


def attend(state, query_rows, qpos, piece, kpos):
    peak, total, accum = state
    rows = piece.shape[1]
    local_heads = query_rows.shape[1]
    pair = piece.reshape(2, rows, local_heads, HEAD_SIZE)
    scores = jnp.einsum(
        "qcgd,kcd->cgqk", query_rows, pair[0], preferred_element_type=jnp.float32
    ) * (1.0 / HEAD_SIZE**0.5)
    allowed = (qpos[:, None] >= kpos[None, :])[None, None]
    scores = jnp.where(allowed, scores, -1e30)
    new_peak = jnp.maximum(peak, jnp.max(scores, axis=-1))
    weights = jnp.where(allowed, jnp.exp(scores - new_peak[..., None]), 0.0)
    factor = jnp.exp(peak - new_peak)
    total = total * factor + jnp.sum(weights, axis=-1)
    update = jnp.einsum(
        "cgqk,kcd->qcgd", weights.astype(jnp.bfloat16), pair[1], preferred_element_type=jnp.float32
    )
    accum = accum * jnp.transpose(factor, (2, 0, 1))[..., None] + update
    return (new_peak, total, accum)


def on_device(hidden, target, gain, w_query, w_key, value_matrix, w_out, block_order):
    rows = hidden.shape[1]
    half = rows // 2
    local = hidden[0]
    whole = lax.all_gather(local, "tp", axis=1, tiled=True)
    wide = whole.astype(jnp.float32)
    normed = (
        wide * lax.rsqrt(jnp.mean(wide * wide, axis=1, keepdims=True) + 1e-05) * gain[None, :]
    ).astype(jnp.bfloat16)
    pieces = (
        lax.all_gather(w_query, ("ctx", "dp"), axis=0, tiled=True),
        lax.all_gather(w_key, ("ctx", "dp"), axis=0, tiled=True),
        lax.all_gather(value_matrix, ("ctx", "dp"), axis=0, tiled=True),
    )
    query_rows, key, value_rows = tuple(
        (jnp.dot(normed, piece, preferred_element_type=jnp.float32) for piece in pieces)
    )
    shard = lax.axis_index("ctx")
    qpos = positions(block_order, shard * rows, rows, half)
    local_heads = w_key.shape[1] // HEAD_SIZE
    query_group = QUERY_HEADS // KEY_VALUE_HEADS
    query_rows = (
        apply_rotary(query_rows.reshape(rows, local_heads * query_group, HEAD_SIZE), qpos)
        .astype(jnp.bfloat16)
        .reshape(rows, local_heads, query_group, HEAD_SIZE)
    )
    key = (
        apply_rotary(key.reshape(rows, local_heads, HEAD_SIZE), qpos)
        .astype(jnp.bfloat16)
        .reshape(rows, local_heads * HEAD_SIZE)
    )
    pair = jnp.stack([key, value_rows.astype(jnp.bfloat16)])
    state = (
        jnp.full((local_heads, query_group, rows), -1e30, jnp.float32),
        jnp.zeros((local_heads, query_group, rows), jnp.float32),
        jnp.zeros((rows, local_heads, query_group, HEAD_SIZE), jnp.float32),
    )
    count = lax.axis_size("ctx")
    state = attend(state, query_rows, qpos, pair, qpos)

    def turn(step, carry):
        moved, inner = carry
        moved = shifted(moved, "ctx", 1)
        source = (shard - step) % count
        return (
            moved,
            attend(
                inner, query_rows, qpos, moved, positions(block_order, source * rows, rows, half)
            ),
        )

    moved_end, state = lax.fori_loop(1, count, turn, (pair, state))
    peak, total, accum = state
    attn = (
        (accum / jnp.transpose(total, (2, 0, 1))[..., None])
        .astype(jnp.bfloat16)
        .reshape(rows, local_heads * query_group * HEAD_SIZE)
    )
    terms = jnp.dot(
        attn,
        lax.all_gather(w_out, ("ctx", "dp"), axis=1, tiled=True),
        preferred_element_type=jnp.float32,
    )
    summed = lax.psum_scatter(terms.astype(jnp.bfloat16), "tp", scatter_dimension=1, tiled=True)
    resid = local.astype(jnp.float32) + summed.astype(jnp.float32) - target[0].astype(jnp.float32)
    squares = lax.psum(jnp.sum(resid * resid), ("ctx", "tp", "dp"))
    loss = squares / (lax.axis_size("dp") * lax.axis_size("ctx") * rows * MODEL_WIDTH)
    return (summed[None], loss)


MESH = pl.DeviceIdType.MESH
F32 = jnp.float32
BF16 = jnp.bfloat16


def layer(
    nd,
    order,
    hidden,
    target,
    gain,
    freqs,
    w_query,
    w_key,
    value_matrix,
    w_out,
    out,
    loss,
    ga,
    go,
    xs,
    goal,
    normed,
    acc,
    trig,
    query,
    kv,
    attn,
    kept,
    sent,
    sib,
    ysend,
    yrecv,
    tile,
    sums_tp,
    sums_all,
    load_sem,
    a_send,
    a_recv,
    o_send,
    o_recv,
    h_send,
    h_recv,
    kv_send,
    kv_recv,
    s_send,
    s_recv,
    y_send,
    y_recv,
    t_send,
    t_recv,
    l_send,
    l_recv,
):
    c, t, d = lax.axis_index("ctx"), lax.axis_index("tp"), lax.axis_index("dp")
    nb = 2 * nd
    me = c * nd + d
    y, k = t // 2, t % 2
    sibling = y * 2 + (1 - k)
    across = (1 - y) * 2 + k
    diagonal = (1 - y) * 2 + (1 - k)
    rows, wide = hidden.shape
    deep = w_query.shape[0]
    qcols = w_query.shape[1]
    half = rows // 2
    n_heads = qcols // HEAD_SIZE
    e = d + 1 - 2 * (d % 2)

    loads = [
        pltpu.make_async_copy(w_query, ga.at[me, :, pl.ds(0, qcols)], load_sem.at[0]),
        pltpu.make_async_copy(w_key, ga.at[me, :, pl.ds(qcols, HEAD_SIZE)], load_sem.at[1]),
        pltpu.make_async_copy(
            value_matrix, ga.at[me, :, pl.ds(qcols + HEAD_SIZE, HEAD_SIZE)], load_sem.at[2]
        ),
        pltpu.make_async_copy(hidden, xs.at[t], load_sem.at[3]),
        pltpu.make_async_copy(w_out, go.at[me], load_sem.at[4]),
        pltpu.make_async_copy(target, goal, load_sem.at[5]),
    ]
    for load in loads:
        load.start()

    barrier = pltpu.get_barrier_semaphore()
    for s in range(1, nb):
        p = (me + s) % nb
        pl.semaphore_signal(
            barrier, inc=1, device_id={"ctx": p // nd, "dp": p % nd}, device_id_type=MESH
        )
    for s in (sibling, across, diagonal):
        pl.semaphore_signal(barrier, inc=1, device_id={"tp": s}, device_id_type=MESH)
    pl.semaphore_wait(barrier, nb + 2)

    def remote(src, dst, ssem, rsem, where):
        return pltpu.make_async_remote_copy(
            src_ref=src, dst_ref=dst, send_sem=ssem, recv_sem=rsem,
            device_id=where, device_id_type=MESH,
        )

    X, UP, DOWN = 0, 1, 2

    def piece(buf, ssem, rsem, b, way):
        where = {
            X: {"ctx": 1 - c},
            UP: {"dp": jnp.minimum(d + 1, nd - 1)},
            DOWN: {"dp": jnp.maximum(d - 1, 0)},
        }[way]
        return remote(buf.at[b], buf.at[b], ssem.at[way, b], rsem.at[b], where)

    def a_piece(b, way):
        return piece(ga, a_send, a_recv, b, way)

    def o_piece(b, way):
        return piece(go, o_send, o_recv, b, way)

    def block(src, j, dst, i, ssem, rsem, where):
        return remote(src.at[j], dst.at[i], ssem, rsem, {"tp": where})

    def h_copy(slot, i, where):
        return block(xs, slot, xs, slot, h_send.at[i], h_recv.at[i], where)

    h_sib = h_copy(t, 0, sibling)
    h_across = h_copy(t, 1, across)
    h_relay = h_copy(across, 2, sibling)
    for i in range(3):
        loads[i].wait()
    a_piece(me, X).start()
    up, down = d < nd - 1, d > 0

    @pl.when(up)
    def _():
        a_piece(me, UP).start()

    @pl.when(down)
    def _():
        a_piece(me, DOWN).start()

    loads[3].wait()
    h_across.start()
    h_sib.start()
    loads[4].wait()
    loads[5].wait()

    def positions_of(shard, index):
        low = order[2 * shard] * half
        high = order[2 * shard + 1] * half
        return jnp.where(index < half, low + index, high + index - half)

    place = positions_of(c, lax.broadcasted_iota(jnp.int32, (rows, HEAD_SIZE), 0)).astype(F32)
    angle = place * freqs[...]
    lane = lax.broadcasted_iota(jnp.int32, (rows, HEAD_SIZE), 1)
    trig[0] = jnp.cos(angle)
    sine = jnp.sin(angle)
    trig[1] = jnp.where(lane < HEAD_SIZE // 2, -sine, sine)

    def relay_a(s):
        @pl.when(d >= s)
        def _():
            b = me - s
            a_piece(b, DOWN).wait_recv()
            a_piece(b, X).start()

            @pl.when(up)
            def _():
                a_piece(b, UP).start()

        @pl.when(d + s < nd)
        def _():
            b = me + s
            a_piece(b, UP).wait_recv()
            a_piece(b, X).start()

            @pl.when(down)
            def _():
                a_piece(b, DOWN).start()

    relay_a(1)

    h_copy(across, 1, across).wait_recv()
    h_relay.start()
    h_copy(sibling, 0, sibling).wait_recv()
    h_copy(diagonal, 2, sibling).wait_recv()
    tp = xs.shape[0]
    chunk = 64
    per = wide // deep

    def norm_rows(i, carry):
        r = pl.multiple_of(i * chunk, chunk)
        total = jnp.zeros((chunk, 1), F32)
        for j in range(tp):
            v = xs[j, pl.ds(r, chunk), :].astype(F32)
            total = total + jnp.sum(v * v, axis=1, keepdims=True)
        scale = lax.rsqrt(total * (1.0 / (tp * wide)) + 1e-05)
        for j in range(tp):
            for m in range(per):
                v = xs[j, pl.ds(r, chunk), m * deep : (m + 1) * deep].astype(F32)
                g = gain[:, j * wide + m * deep : j * wide + (m + 1) * deep]
                normed[j * per + m, pl.ds(r, chunk), :] = (v * scale * g).astype(BF16)
        return carry

    lax.fori_loop(0, rows // chunk, norm_rows, 0)

    for s in range(2, nd):
        relay_a(s)
        if s == nd - 2:

            @pl.when(up)
            def _():
                o_piece(me, UP).start()

            @pl.when(down)
            def _():
                o_piece(me, DOWN).start()

    acc[...] = jnp.zeros_like(acc)

    def project(b):
        acc[...] += jnp.dot(normed[b], ga[b], preferred_element_type=F32)

    def own_line(i, carry):
        project(c * nd + i)
        return carry

    lax.fori_loop(0, nd, own_line, 0)

    def relay_o_line(s):
        @pl.when(d >= s)
        def _():
            b = me - s
            o_piece(b, DOWN).wait_recv()

            @pl.when(up)
            def _():
                o_piece(b, UP).start()

        @pl.when(d + s < nd)
        def _():
            b = me + s
            o_piece(b, UP).wait_recv()

            @pl.when(down)
            def _():
                o_piece(b, DOWN).start()

    def relay_o_x(s):
        @pl.when((d >= s) & (d - s != e))
        def _():
            o_piece(me - s, X).start()

        @pl.when((d + s < nd) & (d + s != e))
        def _():
            o_piece(me + s, X).start()

    relay_o_line(1)

    def other_line(i, carry):
        far = jnp.where(d < nd // 2, i, nd - 1 - i)
        b = (1 - c) * nd + far
        a_piece(b, X).wait_recv()
        project(b)
        return carry

    lax.fori_loop(0, nd, other_line, 0)

    def rotated(v):
        return (v * trig[0] + pltpu.roll(v, HEAD_SIZE // 2, 1) * trig[1]).astype(BF16)

    kv[c, :, 0:HEAD_SIZE] = rotated(acc[:, qcols : qcols + HEAD_SIZE])
    kv[c, :, HEAD_SIZE:] = acc[:, qcols + HEAD_SIZE :].astype(BF16)
    kv_copy = remote(kv.at[c], kv.at[c], kv_send.at[0], kv_recv.at[0], {"ctx": 1 - c})
    kv_copy.start()
    o_piece(me, X).start()
    relay_o_x(1)
    for h in range(n_heads):
        part = slice(h * HEAD_SIZE, (h + 1) * HEAD_SIZE)
        query[h] = rotated(acc[:, part])
    for s in range(2, nd - 1):
        relay_o_line(s)
        relay_o_x(s)

    remote(kv.at[1 - c], kv.at[1 - c], kv_send.at[0], kv_recv.at[0], {"ctx": 1 - c}).wait_recv()
    qrows = 256
    dims = (((1,), (1,)), ((), ()))

    def attend_block(i, carry):
        h = i // (rows // qrows)
        r = pl.multiple_of((i % (rows // qrows)) * qrows, qrows)
        q = query[h, pl.ds(r, qrows), :]
        qpos = positions_of(c, r + lax.broadcasted_iota(jnp.int32, (qrows, rows), 0))
        scores = []
        for n in range(2):
            kpos = positions_of(n, lax.broadcasted_iota(jnp.int32, (qrows, rows), 1))
            sc = lax.dot_general(
                q, kv[n, :, 0:HEAD_SIZE], dims, preferred_element_type=F32
            ) * (1.0 / HEAD_SIZE**0.5)
            scores.append(jnp.where(qpos >= kpos, sc, -1e30))
        peak = jnp.maximum(
            jnp.max(scores[0], axis=1, keepdims=True), jnp.max(scores[1], axis=1, keepdims=True)
        )
        total = jnp.zeros((qrows, 1), F32)
        value = jnp.zeros((qrows, HEAD_SIZE), F32)
        for n in range(2):
            p = jnp.exp(scores[n] - peak)
            total = total + jnp.sum(p, axis=1, keepdims=True)
            value = value + jnp.dot(
                p.astype(BF16), kv[n, :, HEAD_SIZE:], preferred_element_type=F32
            )
        attn[h, pl.ds(r, qrows), :] = (value / total).astype(BF16)
        return carry

    lax.fori_loop(0, n_heads * (rows // qrows), attend_block, 0)

    for s in range(max(2, nd - 1), nd):
        relay_o_line(s)
        relay_o_x(s)

    mirror = (1 - c) * nd + d
    o_piece(mirror, X).wait_recv()

    @pl.when(d % 2 == 0)
    def _():
        o_piece(mirror, UP).start()

    @pl.when(d % 2 == 1)
    def _():
        o_piece(mirror, DOWN).start()

    js = nd // 2

    def out_block(b):
        full = jnp.concatenate([attn[h] for h in range(n_heads)], axis=1)
        return jnp.dot(full, go[b], preferred_element_type=F32).astype(BF16)

    def s_copy(side, j):
        i = side * js + j
        return block(sent, i, sib, i, s_send.at[i], s_recv.at[i], sibling)

    def y_copy(j):
        return block(ysend, j, yrecv, j, y_send.at[j], y_recv.at[j], across)

    near = d < js

    def arrival(i):
        pair, r = i // 2, i % 2
        group = (d // 2 + pair) % js
        mine = jnp.where(r == 0, d, e)
        return jnp.where(pair == 0, mine, group * 2 + jnp.where(near, r, 1 - r))

    for phase in range(2):
        side = c if phase == 0 else 1 - c

        def columns(i, carry):
            within = arrival(i)
            if phase == 1:

                @pl.when(within != d)
                def _():
                    o_piece(side * nd + within, X).wait_recv()

            j = within % js
            slot = side * js + j
            value = out_block(side * nd + within)
            own = within // js == k

            @pl.when(jnp.logical_not(own))
            def _():
                sent[slot] = value
                s_copy(side, j).start()

            @pl.when(own)
            def _():
                kept[slot] = value
                s_copy(side, j).wait_recv()

                @pl.when(side != y)
                def _():
                    ysend[j] = (kept[slot].astype(F32) + sib[slot].astype(F32)).astype(BF16)
                    y_copy(j).start()

            return carry

        lax.fori_loop(0, nd, columns, 0)

    cols = w_out.shape[1]
    tile[...] = jnp.zeros_like(tile)
    def finish_block(n, carry):
        j = jnp.where(near, n, js - 1 - n)
        y_copy(j).wait_recv()
        place = pl.ds(pl.multiple_of(j * cols, cols), cols)
        mine = y * js + j

        def finish(i, inner):
            rr = pl.ds(pl.multiple_of(i * chunk, chunk), chunk)
            total = (
                kept[mine, rr, :].astype(F32) + sib[mine, rr, :].astype(F32)
            ) + yrecv[j, rr, :].astype(F32)
            result = total.astype(BF16)
            out[rr, place] = result
            resid = xs[t, rr, place].astype(F32) + result.astype(F32)
            resid = resid - goal[rr, place].astype(F32)
            sq = jnp.sum((resid * resid).reshape(chunk // 8, 8, cols), axis=0)
            part = sq[:, 0:128]
            for m in range(1, cols // 128):
                part = part + sq[:, m * 128 : (m + 1) * 128]
            tile[...] += part
            return inner

        lax.fori_loop(0, rows // chunk, finish, 0)
        return carry

    lax.fori_loop(0, js, finish_block, 0)

    sums_tp[0] = tile[...]
    tp_copies = [
        block(sums_tp, 0, sums_tp, 1 + i, t_send.at[i], t_recv.at[i], where)
        for i, where in enumerate((sibling, across, diagonal))
    ]
    for copy in tp_copies:
        copy.start()
    for copy in tp_copies:
        copy.wait_recv()
    sums_all[me] = (sums_tp[0] + sums_tp[1]) + (sums_tp[2] + sums_tp[3])

    def l_copy(s, slot):
        p = (me + s) % nb
        return remote(
            sums_all.at[slot], sums_all.at[slot], l_send.at[s], l_recv.at[slot],
            {"ctx": p // nd, "dp": p % nd},
        )

    for s in range(1, nb):
        l_copy(s, me).start()
    for s in range(1, nb):
        l_copy(s, (me + s) % nb).wait_recv()
    whole = sums_all[0]
    for b in range(1, nb):
        whole = whole + sums_all[b]
    count = tp * wide * rows * nb
    loss[0, 0] = jnp.sum(whole) / count

    h_across.wait_send()
    h_sib.wait_send()
    h_relay.wait_send()
    kv_copy.wait_send()
    for copy in tp_copies:
        copy.wait_send()
    for s in range(1, nb):
        l_copy(s, me).wait_send()
    for side in range(2):
        for j in range(js):
            s_copy(side, j).wait_send()
    for j in range(js):
        y_copy(j).wait_send()
    a_piece(me, X).wait_send()
    o_piece(me, X).wait_send()
    for s in range(0, nd):
        for sign in (-1, 1) if s else (1,):
            b = me + sign * s
            there = (d + sign * s >= 0) & (d + sign * s < nd)
            if s:

                @pl.when(there)
                def _():
                    a_piece(b, X).wait_send()

                @pl.when(there & (d + sign * s != e))
                def _():
                    o_piece(b, X).wait_send()

            if s == 0 or sign < 0:

                @pl.when(there & up)
                def _():
                    a_piece(b, UP).wait_send()
                    o_piece(b, UP).wait_send()

            if s == 0 or sign > 0:

                @pl.when(there & down)
                def _():
                    a_piece(b, DOWN).wait_send()
                    o_piece(b, DOWN).wait_send()

    @pl.when(d % 2 == 0)
    def _():
        o_piece(mirror, UP).wait_send()

    @pl.when(d % 2 == 1)
    def _():
        o_piece(mirror, DOWN).wait_send()


def fused(nd, hidden, target, gain, w_query, w_key, value_matrix, w_out, block_order):
    rows, wide = hidden.shape[1:]
    nb = 2 * nd
    tp = lax.axis_size("tp")
    deep, qcols = w_query.shape
    all_cols = qcols + w_key.shape[1] + value_matrix.shape[1]
    orows, ocols = w_out.shape
    half = HEAD_SIZE // 2
    freqs = rope_base ** (-(jnp.arange(half, dtype=F32) * 2.0) / HEAD_SIZE)
    freqs = jnp.concatenate([freqs, freqs])[None, :]
    heads = qcols // HEAD_SIZE
    js = nd // 2
    vmem = pl.BlockSpec(memory_space=pltpu.VMEM)
    anyspace = pl.BlockSpec(memory_space=pl.ANY)
    dma = pltpu.SemaphoreType.DMA
    branch, loss = pl.pallas_call(
        functools.partial(layer, nd),
        out_shape=(
            jax.ShapeDtypeStruct((rows, wide), BF16),
            jax.ShapeDtypeStruct((1, 1), F32),
        ),
        in_specs=[
            pl.BlockSpec(memory_space=pltpu.SMEM),
            anyspace,
            anyspace,
            vmem,
            vmem,
            anyspace,
            anyspace,
            anyspace,
            anyspace,
        ],
        out_specs=(vmem, pl.BlockSpec(memory_space=pltpu.SMEM)),
        scratch_shapes=[
            pltpu.VMEM((nb, deep, all_cols), BF16),
            pltpu.VMEM((nb, orows, ocols), BF16),
            pltpu.VMEM((tp, rows, wide), BF16),
            pltpu.VMEM((rows, wide), BF16),
            pltpu.VMEM((nb, rows, deep), BF16),
            pltpu.VMEM((rows, all_cols), F32),
            pltpu.VMEM((2, rows, HEAD_SIZE), F32),
            pltpu.VMEM((heads, rows, HEAD_SIZE), BF16),
            pltpu.VMEM((2, rows, 2 * HEAD_SIZE), BF16),
            pltpu.VMEM((heads, rows, HEAD_SIZE), BF16),
            pltpu.VMEM((2 * js, rows, ocols), BF16),
            pltpu.VMEM((2 * js, rows, ocols), BF16),
            pltpu.VMEM((2 * js, rows, ocols), BF16),
            pltpu.VMEM((js, rows, ocols), BF16),
            pltpu.VMEM((js, rows, ocols), BF16),
            pltpu.VMEM((8, 128), F32),
            pltpu.VMEM((tp, 8, 128), F32),
            pltpu.VMEM((nb, 8, 128), F32),
            dma((6,)),
            dma((3, nb)),
            dma((nb,)),
            dma((3, nb)),
            dma((nb,)),
            dma((3,)),
            dma((3,)),
            dma((1,)),
            dma((1,)),
            dma((2 * js,)),
            dma((2 * js,)),
            dma((js,)),
            dma((js,)),
            dma((3,)),
            dma((3,)),
            dma((nb,)),
            dma((nb,)),
        ],
        compiler_params=pltpu.CompilerParams(
            collective_id=1, has_side_effects=True, vmem_limit_bytes=60 * 1024 * 1024
        ),
    )(
        block_order,
        hidden[0],
        target[0],
        gain[None, :],
        freqs,
        w_query,
        w_key,
        value_matrix,
        w_out,
    )
    return (branch[None], loss.reshape(()))


def solution(mesh):
    in_specs = (
        P("dp", "ctx", "tp"),
        P("dp", "ctx", "tp"),
        P(),
        P(("ctx", "dp"), "tp"),
        P(("ctx", "dp"), "tp"),
        P(("ctx", "dp"), "tp"),
        P("tp", ("ctx", "dp")),
        P(),
    )
    out_specs = (P("dp", "ctx", "tp"), P())
    sizes = mesh.shape
    fits = sizes["ctx"] == 2 and sizes["tp"] == 4 and sizes["dp"] % 2 == 0
    body = functools.partial(fused, sizes["dp"]) if fits else on_device
    return jax.shard_map(
        body, mesh=mesh, in_specs=in_specs, out_specs=out_specs, check_vma=False
    )
```
